32 devices in a mesh: dp: 8 (over z, y), mp: 4 (over x, core).
Axes of the slice: x: 2, y: 2, z: 4, core: 2. Of those that a mesh axis runs over, the one named last changes fastest.
Arguments:
- documents: bfloat16 [16384, 1024], P('dp', 'mp'), may hold values from -6 to 6
- assign: int32 [16384], P('dp'), may hold values from 0 to 4095, as said below
- quality: float32 [16384], P('dp'), may hold values from 0.1 to 1
- centroids: bfloat16 [4096, 1024], P('mp'), may hold values from -6 to 6
Outputs:
- distances: float32 [16384], P('dp')
- new_centroids: bfloat16 [4096, 1024], P('dp', 'mp')
- cluster_quality: float32 [4096], P('dp')
- inertia: float32 [], replicated
The draws below stay inside these ranges and needn't reach their ends.
Inputs may be any that keep to these rules, and one draw needn't show every extreme that they name: `assign`: call the clusters o * 512 to (o + 1) * 512 - 1 those of owner o. Among each run of 2048 documents held by one index of dp, at most 512 have clusters of any one owner, and one owner, the same for every index, gets exactly 512 of them from every index.
All inputs are finite; a program needn't handle non-finite values.
Results may differ from the reference program's by a relative error of at most 0.0044.
Values may be sent and summed in bfloat16 or wider, within the bound.
A program may use at most 64 MiB of HBM per device.

```python
import math
import jax
import jax.numpy as jnp

D = 1024
K = 4096
ROWS_DEV = 2048
DOCS = 16384
N_DP = 8


def draw_assign(key, part):
    owned = K // N_DP
    capacity = max(2, 2 * ROWS_DEV // N_DP)
    common = jax.random.randint(jax.random.fold_in(key, 7), (), 0, N_DP).astype(jnp.int32)

    def one_device(index):
        subkey = jax.random.fold_in(key, index + 100)
        key_one, key_two, key_three = jax.random.split(subkey, 3)
        others = (jnp.arange((N_DP - 1) * capacity, dtype=jnp.int32) // capacity).astype(jnp.int32)
        others = jnp.where(others >= common, others + 1, others)
        mixed = jax.random.permutation(key_one, others)
        owners = jnp.concatenate([jnp.zeros((capacity,), jnp.int32) + common, mixed[:ROWS_DEV - capacity]])
        owners = jax.random.permutation(key_two, owners)
        inside = jax.random.randint(key_three, (ROWS_DEV,), 0, owned).astype(jnp.int32)
        return (owners * owned + inside).astype(jnp.int32)
    return jax.vmap(one_device)(jnp.arange(N_DP, dtype=jnp.int32)).reshape(-1)


def levels(own_key, extent, pieces, smallest, top_value):
    loudness, own = 1.0, jax.random.fold_in(own_key, 6)
    for dim, blocks in pieces:
        draws = jnp.exp(jax.random.uniform(jax.random.fold_in(own, dim), (blocks,), jnp.float32, smallest / len(pieces), top_value / len(pieces)))
        loudness = loudness * jnp.repeat(draws, extent[dim] // blocks).reshape([-1 if axis == dim else 1 for axis in range(len(extent))])
    return loudness


def bell_draw(stream_key, shape, deviation, bound, cuts=(), kind=jnp.bfloat16):
    drawn = deviation * jax.random.normal(stream_key, shape, jnp.float32)
    if cuts:
        drawn = drawn * levels(stream_key, shape, cuts, -0.22, 0.18)
    return jnp.clip(drawn, -bound, bound).astype(kind)


def setup_inputs(seed: int = 0) -> dict:
    key_list = jax.random.split(jax.random.key(seed), 5)
    return {
        "documents": bell_draw(key_list[0], (DOCS, D), 1.0, 6.0, ((0, 8), (1, 4))),
        "assign": draw_assign(jax.random.fold_in(key_list[4], 71), 0),
        "quality": jnp.clip(jnp.exp(math.log(1.0) - 2.3025851 * jax.random.uniform(key_list[2], (DOCS,), jnp.float32) ** levels(key_list[2], (DOCS,), ((0, 8),), -0.2, 0.2)), 0.1, 1.0),
        "centroids": bell_draw(key_list[3], (K, D), 1.0, 6.0, ((0, 4),)),
    }


def reference(documents, assign, quality, centroids):
    values = documents.astype(jnp.float32)
    picked = centroids[assign].astype(jnp.float32)
    diff = values - picked
    distances = jnp.sum(diff * diff, axis=1) / D
    inertia = jnp.sum(distances) / DOCS
    weight = quality.astype(jnp.bfloat16).astype(jnp.float32)
    sums = jax.ops.segment_sum(weight[:, None] * values, assign, num_segments=K)
    counts = jax.ops.segment_sum(jnp.ones_like(weight), assign, num_segments=K)
    mass = jax.ops.segment_sum(weight, assign, num_segments=K)
    new_centroids = ((sums + centroids.astype(jnp.float32)) / (mass + 1.0)[:, None]).astype(jnp.bfloat16)
    cluster_quality = mass / (counts + 1.0)
    return distances, new_centroids, cluster_quality, inertia
```

```python
import functools

import jax
import jax.numpy as jnp
from jax import lax
from jax.experimental import pallas as pl
from jax.experimental.pallas import tpu as pltpu
from jax.sharding import PartitionSpec as P

MESH = pl.DeviceIdType.MESH
LANES = 128
CHUNKS = 4


def kernel(
    n_dp, n_mp, assign_ref, quality_ref, docs_ref, cents_ref,
    dist_ref, new_ref, cq_ref, inertia_ref,
    fc, acc, acol, own, ysend, ybuf, zsend, zbuf, ag, qg, dbuf, ibuf, isend,
    a_ss, a_rs, a_ls, g_ss, g_rs, y_ss, y_rs, z_ss, z_rs, d_ss, d_rs, i_ss, i_rs,
):
    f32, bf16 = jnp.float32, jnp.bfloat16
    dp, mp = lax.axis_index("dp"), lax.axis_index("mp")
    n_hi = n_dp // 2
    hi, lo = dp // 2, dp % 2
    rows, width = docs_ref.shape
    depth = cents_ref.shape[0]
    share = new_ref.shape[0]
    nb = rows // LANES
    clen = depth // CHUNKS

    barrier = pltpu.get_barrier_semaphore()
    for s in range(1, n_mp):
        pl.semaphore_signal(barrier, inc=1, device_id={"mp": (mp + s) % n_mp}, device_id_type=MESH)

    @pl.loop(1, n_dp)
    def _(s):
        pl.semaphore_signal(barrier, inc=1, device_id={"dp": (dp + s) % n_dp}, device_id_type=MESH)

    pl.semaphore_wait(barrier, n_mp - 1 + n_dp - 1)

    def cent_copy(peer, slot, c):
        cols = pl.ds(pl.multiple_of(peer * width, LANES), width)
        return pltpu.make_async_remote_copy(
            src_ref=cents_ref.at[pl.ds(c * clen, clen), cols],
            dst_ref=fc.at[slot, pl.ds(c * clen, clen), :],
            send_sem=a_ss.at[peer, c],
            recv_sem=a_rs.at[slot, c],
            device_id={"mp": peer},
            device_id_type=MESH,
        )

    near = mp + 1 - 2 * (mp % 2)
    fars = [(d + 2 * s) % n_mp for s in range(1, n_mp // 2) for d in (mp, near)]
    peers = [near] + fars
    for c in range(CHUNKS):
        for peer in fars:
            cent_copy(peer, mp, c).start()
    for c in range(CHUNKS):
        cent_copy(near, mp, c).start()
    mine = pltpu.make_async_copy(
        cents_ref.at[:, pl.ds(pl.multiple_of(mp * width, LANES), width)], fc.at[mp], a_ls
    )
    mine.start()

    def gather_copies(peer, slot):
        return [
            pltpu.make_async_remote_copy(
                src_ref=src, dst_ref=dst.at[slot], send_sem=g_ss.at[i, peer],
                recv_sem=g_rs.at[i, slot], device_id={"dp": peer}, device_id_type=MESH,
            )
            for i, (src, dst) in enumerate(((assign_ref, ag), (quality_ref, qg)))
        ]

    @pl.loop(1, n_dp)
    def _(s):
        for copy in gather_copies((dp + s) % n_dp, dp):
            copy.start()

    row_iota = lax.broadcasted_iota(jnp.int32, (share, LANES), 0)

    def partial(owner):
        base = owner * share
        pieces = []
        for b in range(nb):
            hit = (assign_ref[pl.ds(b, 1), :] - base) == row_iota
            pieces.append(jnp.where(hit, quality_ref[pl.ds(b, 1), :], 0.0).astype(bf16))
        weighted = jnp.concatenate(pieces, axis=1)
        return jnp.dot(weighted, docs_ref[...], preferred_element_type=f32)

    def y_copy(h):
        return pltpu.make_async_remote_copy(
            src_ref=ysend.at[h], dst_ref=ybuf.at[h], send_sem=y_ss.at[h], recv_sem=y_rs.at[h],
            device_id={"dp": hi * 2 + 1 - lo}, device_id_type=MESH,
        )

    @pl.loop(0, n_hi)
    def _(k):
        h = (hi + 1 + k) % n_hi
        ysend[h] = partial(h * 2 + 1 - lo).astype(bf16)
        y_copy(h).start()

    @pl.loop(0, n_hi)
    def _(k):
        h = (hi + 1 + k) % n_hi
        own[h] = partial(h * 2 + lo)

    def z_copy(h, slot):
        return pltpu.make_async_remote_copy(
            src_ref=zsend.at[h], dst_ref=zbuf.at[slot], send_sem=z_ss.at[h], recv_sem=z_rs.at[slot],
            device_id={"dp": h * 2 + lo}, device_id_type=MESH,
        )

    def forward(k):
        h = (hi + 1 + k) % n_hi
        y_copy(h).wait_recv()
        zsend[h] = (own[h] + ybuf[h].astype(f32)).astype(bf16)
        z_copy(h, hi).start()

    for b in range(nb):
        ids = jnp.broadcast_to(assign_ref[pl.ds(b, 1), :].astype(f32), (LANES, LANES))
        acol[pl.ds(b * LANES, LANES), :] = ids.T

    tile = min(512, rows)

    def pick(src, start, size, first=False):
        base = (src * depth + start).astype(f32)

        @pl.loop(0, rows // tile)
        def _(t):
            at = pl.ds(pl.multiple_of(t * tile, tile), tile)
            ids = acol[at, :] - base
            lane = lax.broadcasted_iota(jnp.int32, (tile, LANES), 1)
            onehot = jnp.concatenate(
                [
                    jnp.where(ids == (lane + j * LANES).astype(f32), 1.0, 0.0).astype(bf16)
                    for j in range(size // LANES)
                ],
                axis=1,
            )
            got = jnp.dot(onehot, fc[src, pl.ds(start, size), :], preferred_element_type=f32)
            prior = docs_ref[at, :].astype(f32) if first else acc[at, :]
            acc[at, :] = prior - got

    mine.wait()
    pick(mp, 0, depth, first=True)
    forwards = n_hi - 1
    cut = [forwards * c // (CHUNKS - 1) for c in range(CHUNKS)]
    if CHUNKS > 1:
        pl.loop(cut[0], cut[1])(forward)
    for c in range(CHUNKS):
        cent_copy(near, near, c).wait_recv()
    pick(near, 0, depth)

    lane_len = min(LANES, share)
    groups = share // lane_len
    half = max(4, groups)
    ag[dp] = assign_ref[...]
    qg[dp] = quality_ref[...]

    def count(i, total):
        d = (dp + i) % n_dp

        @pl.when(i > 0)
        def _():
            for copy in gather_copies(d, d):
                copy.wait_recv()

        left, right = [], []
        part = lax.broadcasted_iota(jnp.int32, (2 * half, LANES), 0)
        low = lax.broadcasted_iota(jnp.int32, (lane_len, LANES), 0)
        for b in range(nb):
            ids = ag[d, pl.ds(b, 1), :] - dp * share
            upper = ids >> (lane_len.bit_length() - 1)
            lower = ids & (lane_len - 1)
            weight = jnp.where(part < half, 1.0, qg[d, pl.ds(b, 1), :])
            member = jnp.where(part < half, part, part - half) == upper
            left.append(jnp.where(member, weight, 0.0).astype(bf16))
            right.append(jnp.where(low == lower, 1.0, 0.0).astype(bf16))
        return total + lax.dot_general(
            jnp.concatenate(left, axis=1), jnp.concatenate(right, axis=1),
            (((1,), (1,)), ((), ())), preferred_element_type=f32,
        )

    totals = lax.fori_loop(0, n_dp, count, jnp.zeros((2 * half, lane_len), f32))
    counts, mass = totals[:groups], totals[half : half + groups]
    cq_ref[...] = mass / (counts + 1.0)

    for c in range(CHUNKS):
        for peer in fars:
            cent_copy(peer, peer, c).wait_recv()
            pick(peer, c * clen, clen)
        if c + 2 < CHUNKS:
            pl.loop(cut[c + 1], cut[c + 2])(forward)

    @pl.loop(0, nb)
    def _(b):
        diff = acc[pl.ds(pl.multiple_of(b * LANES, LANES), LANES), :]
        square = diff * diff
        folded = square[:, :LANES]
        for j in range(1, width // LANES):
            folded = folded + square[:, j * LANES : (j + 1) * LANES]
        dbuf[mp, pl.ds(b, 1), :] = jnp.sum(folded.T, axis=0, keepdims=True)

    def d_copy(peer, slot):
        return pltpu.make_async_remote_copy(
            src_ref=dbuf.at[mp], dst_ref=dbuf.at[slot], send_sem=d_ss.at[peer], recv_sem=d_rs.at[slot],
            device_id={"mp": peer}, device_id_type=MESH,
        )

    for peer in peers:
        d_copy(peer, mp).start()
    for peer in peers:
        d_copy(peer, peer).wait_recv()
    dist = dbuf[0]
    for s in range(1, n_mp):
        dist = dist + dbuf[s]
    dist = dist / (width * n_mp)
    dist_ref[...] = dist
    folded = dist[:8]
    for j in range(1, nb // 8):
        folded = folded + dist[j * 8 : (j + 1) * 8]
    isend[...] = folded

    def i_copy(peer, slot):
        return pltpu.make_async_remote_copy(
            src_ref=isend, dst_ref=ibuf.at[slot], send_sem=i_ss.at[peer], recv_sem=i_rs.at[slot],
            device_id={"dp": peer}, device_id_type=MESH,
        )

    @pl.loop(1, n_dp)
    def _(s):
        i_copy((dp + s) % n_dp, dp).start()

    ibuf[dp] = folded

    y_copy(hi).wait_recv()
    own[hi] = own[hi] + ybuf[hi].astype(f32)

    @pl.loop(1, n_hi)
    def _(s):
        h = (hi + s) % n_hi
        z_copy(h, h).wait_recv()
        own[hi] = own[hi] + zbuf[h].astype(f32)

    first = dp * share
    src, start = first // depth, first % depth
    for g in range(groups):
        column = jnp.broadcast_to(mass[g : g + 1, :], (LANES, lane_len)).T + 1.0
        column = jnp.concatenate([column] * (width // LANES), axis=1)
        at = pl.ds(g * lane_len, lane_len)
        old = fc[src, pl.ds(pl.multiple_of(start + g * lane_len, lane_len), lane_len), :].astype(f32)
        new_ref[at, :] = ((own[hi, at, :] + old) / column).astype(bf16)

    @pl.loop(1, n_dp)
    def _(s):
        d = (dp + s) % n_dp
        i_copy(d, d).wait_recv()

    total = lax.fori_loop(1, n_dp, lambda d, t: t + ibuf[d], ibuf[0])
    inertia_ref[0, 0] = jnp.sum(total) / (rows * n_dp)

    for peer in peers:
        d_copy(peer, mp).wait_send()
        for c in range(CHUNKS):
            cent_copy(peer, mp, c).wait_send()

    @pl.loop(1, n_dp)
    def _(s):
        d = (dp + s) % n_dp
        i_copy(d, dp).wait_send()
        for copy in gather_copies(d, dp):
            copy.wait_send()

    @pl.loop(0, n_hi)
    def _(h):
        y_copy(h).wait_send()

    @pl.loop(1, n_hi)
    def _(s):
        z_copy((hi + s) % n_hi, hi).wait_send()


def per_device(n_dp, n_mp, documents, assign, quality, centroids):
    rows, width = documents.shape
    depth = centroids.shape[0]
    share = depth * n_mp // n_dp
    nb = rows // LANES
    n_hi = n_dp // 2
    lane_len = min(LANES, share)
    f32, bf16 = jnp.float32, jnp.bfloat16
    vmem = pl.BlockSpec(memory_space=pltpu.VMEM)
    dma = pltpu.SemaphoreType.DMA
    dist, new, cq, inertia = pl.pallas_call(
        functools.partial(kernel, n_dp, n_mp),
        out_shape=(
            jax.ShapeDtypeStruct((nb, LANES), f32),
            jax.ShapeDtypeStruct((share, width), bf16),
            jax.ShapeDtypeStruct((share // lane_len, lane_len), f32),
            jax.ShapeDtypeStruct((1, 1), f32),
        ),
        in_specs=[vmem, vmem, vmem, pl.BlockSpec(memory_space=pl.ANY)],
        out_specs=(vmem, vmem, vmem, pl.BlockSpec(memory_space=pltpu.SMEM)),
        scratch_shapes=[
            pltpu.VMEM((n_mp, depth, width), bf16),
            pltpu.VMEM((rows, width), f32),
            pltpu.VMEM((rows, LANES), f32),
            pltpu.VMEM((n_hi, share, width), f32),
            pltpu.VMEM((n_hi, share, width), bf16),
            pltpu.VMEM((n_hi, share, width), bf16),
            pltpu.VMEM((n_hi, share, width), bf16),
            pltpu.VMEM((n_hi, share, width), bf16),
            pltpu.VMEM((n_dp, nb, LANES), jnp.int32),
            pltpu.VMEM((n_dp, nb, LANES), f32),
            pltpu.VMEM((n_mp, nb, LANES), f32),
            pltpu.VMEM((n_dp, 8, LANES), f32),
            pltpu.VMEM((8, LANES), f32),
            dma((n_mp, CHUNKS)), dma((n_mp, CHUNKS)), dma,
            dma((2, n_dp)), dma((2, n_dp)),
            dma((n_hi,)), dma((n_hi,)),
            dma((n_hi,)), dma((n_hi,)),
            dma((n_mp,)), dma((n_mp,)),
            dma((n_dp,)), dma((n_dp,)),
        ],
        compiler_params=pltpu.CompilerParams(
            collective_id=0, has_side_effects=True, vmem_limit_bytes=48 * 2**20
        ),
    )(assign.reshape(nb, LANES), quality.reshape(nb, LANES), documents, centroids)
    return dist.reshape(rows), new, cq.reshape(share), inertia.reshape(())


def solution(mesh):
    return jax.shard_map(
        functools.partial(per_device, mesh.shape["dp"], mesh.shape["mp"]),
        mesh=mesh,
        in_specs=(P("dp", "mp"), P("dp"), P("dp"), P("mp", None)),
        out_specs=(P("dp"), P("dp", "mp"), P("dp"), P()),
        check_vma=False,
    )
```

```python
import functools

import jax
import jax.numpy as jnp
from jax import lax
from jax.experimental import pallas as pl
from jax.experimental.pallas import tpu as pltpu
from jax.sharding import PartitionSpec as P

MESH = pl.DeviceIdType.MESH
LANES = 128
CHUNKS = 4
PARTS = 2


def kernel(
    n_dp, n_mp, assign_hbm, quality_hbm, docs_hbm, cents_ref,
    dist_ref, new_ref, cq_ref, inertia_ref,
    assign_ref, quality_ref, docs_ref, fc, acc, acol, own, ysend, ybuf, zsend, zbuf, ag, qg, dbuf, ibuf, isend,
    in_sems, a_ss, a_rs, a_ls, g_ss, g_rs, y_ss, y_rs, z_ss, z_rs, d_ss, d_rs, i_ss, i_rs,
):
    f32, bf16 = jnp.float32, jnp.bfloat16
    dp, mp = lax.axis_index("dp"), lax.axis_index("mp")
    n_hi = n_dp // 2
    hi, lo = dp // 2, dp % 2
    rows, width = docs_ref.shape
    depth = cents_ref.shape[0]
    share = new_ref.shape[0]
    nb = rows // LANES
    clen = depth // CHUNKS

    loads = [
        pltpu.make_async_copy(src, dst, in_sems.at[i])
        for i, (src, dst) in enumerate(
            ((assign_hbm, assign_ref), (quality_hbm, quality_ref), (docs_hbm, docs_ref))
        )
    ]
    for load in loads:
        load.start()

    barrier = pltpu.get_barrier_semaphore()
    for s in range(1, n_mp):
        pl.semaphore_signal(barrier, inc=1, device_id={"mp": (mp + s) % n_mp}, device_id_type=MESH)

    @pl.loop(1, n_dp)
    def _(s):
        pl.semaphore_signal(barrier, inc=1, device_id={"dp": (dp + s) % n_dp}, device_id_type=MESH)

    pl.semaphore_wait(barrier, n_mp - 1 + n_dp - 1)

    def cent_copy(peer, slot, c):
        cols = pl.ds(pl.multiple_of(peer * width, LANES), width)
        return pltpu.make_async_remote_copy(
            src_ref=cents_ref.at[pl.ds(c * clen, clen), cols],
            dst_ref=fc.at[slot, pl.ds(c * clen, clen), :],
            send_sem=a_ss.at[peer, c],
            recv_sem=a_rs.at[slot, c],
            device_id={"mp": peer},
            device_id_type=MESH,
        )

    near = mp + 1 - 2 * (mp % 2)
    fars = [(d + 2 * s) % n_mp for s in range(1, n_mp // 2) for d in (mp, near)]
    peers = [near] + fars
    for c in range(CHUNKS):
        for peer in fars:
            cent_copy(peer, mp, c).start()
    for c in range(CHUNKS):
        cent_copy(near, mp, c).start()
    mine = pltpu.make_async_copy(
        cents_ref.at[:, pl.ds(pl.multiple_of(mp * width, LANES), width)], fc.at[mp], a_ls
    )
    mine.start()
    for load in loads:
        load.wait()

    def gather_copies(peer, slot):
        return [
            pltpu.make_async_remote_copy(
                src_ref=src, dst_ref=dst.at[slot], send_sem=g_ss.at[i, peer],
                recv_sem=g_rs.at[i, slot], device_id={"dp": peer}, device_id_type=MESH,
            )
            for i, (src, dst) in enumerate(((assign_ref, ag), (quality_ref, qg)))
        ]

    @pl.loop(1, n_dp)
    def _(s):
        for copy in gather_copies((dp + s) % n_dp, dp):
            copy.start()

    row_iota = lax.broadcasted_iota(jnp.int32, (share, LANES), 0)

    def partial(owner):
        base = owner * share
        pieces = []
        for b in range(nb):
            hit = (assign_ref[pl.ds(b, 1), :] - base) == row_iota
            pieces.append(jnp.where(hit, quality_ref[pl.ds(b, 1), :], 0.0).astype(bf16))
        weighted = jnp.concatenate(pieces, axis=1)
        return jnp.dot(weighted, docs_ref[...], preferred_element_type=f32)

    part_rows = share // PARTS

    def y_copy(h, p):
        at = pl.ds(pl.multiple_of(p * part_rows, part_rows), part_rows)
        return pltpu.make_async_remote_copy(
            src_ref=ysend.at[h, at], dst_ref=ybuf.at[h, at],
            send_sem=y_ss.at[h, p], recv_sem=y_rs.at[h, p],
            device_id={"dp": hi * 2 + 1 - lo}, device_id_type=MESH,
        )

    @pl.loop(0, n_hi)
    def _(k):
        h = (hi + 1 + k) % n_hi
        ysend[h] = partial(h * 2 + 1 - lo).astype(bf16)
        for p in range(PARTS):
            y_copy(h, p).start()

    @pl.loop(0, n_hi)
    def _(k):
        h = (hi + 1 + k) % n_hi
        own[h] = partial(h * 2 + lo)

    def z_copy(h, slot, p):
        at = pl.ds(pl.multiple_of(p * part_rows, part_rows), part_rows)
        return pltpu.make_async_remote_copy(
            src_ref=zsend.at[h, at], dst_ref=zbuf.at[slot, at],
            send_sem=z_ss.at[h, p], recv_sem=z_rs.at[slot, p],
            device_id={"dp": h * 2 + lo}, device_id_type=MESH,
        )

    def forward(t):
        h, p = (hi + 1 + t // PARTS) % n_hi, t % PARTS
        at = pl.ds(pl.multiple_of(p * part_rows, part_rows), part_rows)
        y_copy(h, p).wait_recv()
        zsend[h, at, :] = (own[h, at, :] + ybuf[h, at, :].astype(f32)).astype(bf16)
        z_copy(h, hi, p).start()

    for b in range(nb):
        ids = jnp.broadcast_to(assign_ref[pl.ds(b, 1), :].astype(f32), (LANES, LANES))
        acol[pl.ds(b * LANES, LANES), :] = ids.T

    tile = min(512, rows)

    def pick(src, start, size, first=False):
        base = (src * depth + start).astype(f32)

        @pl.loop(0, rows // tile)
        def _(t):
            at = pl.ds(pl.multiple_of(t * tile, tile), tile)
            ids = acol[at, :] - base
            lane = lax.broadcasted_iota(jnp.int32, (tile, LANES), 1)
            onehot = jnp.concatenate(
                [
                    jnp.where(ids == (lane + j * LANES).astype(f32), 1.0, 0.0).astype(bf16)
                    for j in range(size // LANES)
                ],
                axis=1,
            )
            got = jnp.dot(onehot, fc[src, pl.ds(start, size), :], preferred_element_type=f32)
            prior = docs_ref[at, :].astype(f32) if first else acc[at, :]
            acc[at, :] = prior - got

    mine.wait()
    pick(mp, 0, depth, first=True)
    forwards = (n_hi - 1) * PARTS
    cut = [forwards * c // 6 for c in (0, 1, 2, 3, 5, 6)]
    pl.loop(cut[0], cut[1])(forward)
    for c in range(CHUNKS):
        cent_copy(near, near, c).wait_recv()
    pick(near, 0, depth)
    pl.loop(cut[1], cut[2])(forward)

    lane_len = min(LANES, share)
    groups = share // lane_len
    half = max(4, groups)
    ag[dp] = assign_ref[...]
    qg[dp] = quality_ref[...]

    def count(i, total):
        d = (dp + i) % n_dp

        @pl.when(i > 0)
        def _():
            for copy in gather_copies(d, d):
                copy.wait_recv()

        left, right = [], []
        part = lax.broadcasted_iota(jnp.int32, (2 * half, LANES), 0)
        low = lax.broadcasted_iota(jnp.int32, (lane_len, LANES), 0)
        for b in range(nb):
            ids = ag[d, pl.ds(b, 1), :] - dp * share
            upper = ids >> (lane_len.bit_length() - 1)
            lower = ids & (lane_len - 1)
            weight = jnp.where(part < half, 1.0, qg[d, pl.ds(b, 1), :])
            member = jnp.where(part < half, part, part - half) == upper
            left.append(jnp.where(member, weight, 0.0).astype(bf16))
            right.append(jnp.where(low == lower, 1.0, 0.0).astype(bf16))
        return total + lax.dot_general(
            jnp.concatenate(left, axis=1), jnp.concatenate(right, axis=1),
            (((1,), (1,)), ((), ())), preferred_element_type=f32,
        )

    totals = lax.fori_loop(0, n_dp, count, jnp.zeros((2 * half, lane_len), f32))
    counts, mass = totals[:groups], totals[half : half + groups]
    cq_ref[...] = mass / (counts + 1.0)
    pl.loop(cut[2], cut[3])(forward)

    for c in range(CHUNKS):
        for peer in fars:
            cent_copy(peer, peer, c).wait_recv()
            pick(peer, c * clen, clen)
        if c < 2:
            pl.loop(cut[c + 3], cut[c + 4])(forward)

    @pl.loop(0, nb)
    def _(b):
        diff = acc[pl.ds(pl.multiple_of(b * LANES, LANES), LANES), :]
        square = diff * diff
        folded = square[:, :LANES]
        for j in range(1, width // LANES):
            folded = folded + square[:, j * LANES : (j + 1) * LANES]
        dbuf[mp, pl.ds(b, 1), :] = jnp.sum(folded.T, axis=0, keepdims=True)

    def d_copy(peer, slot):
        return pltpu.make_async_remote_copy(
            src_ref=dbuf.at[mp], dst_ref=dbuf.at[slot], send_sem=d_ss.at[peer], recv_sem=d_rs.at[slot],
            device_id={"mp": peer}, device_id_type=MESH,
        )

    for peer in peers:
        d_copy(peer, mp).start()
    for peer in peers:
        d_copy(peer, peer).wait_recv()
    dist = dbuf[0]
    for s in range(1, n_mp):
        dist = dist + dbuf[s]
    dist = dist / (width * n_mp)
    dist_ref[...] = dist
    folded = dist[:8]
    for j in range(1, nb // 8):
        folded = folded + dist[j * 8 : (j + 1) * 8]
    isend[...] = folded

    def i_copy(peer, slot):
        return pltpu.make_async_remote_copy(
            src_ref=isend, dst_ref=ibuf.at[slot], send_sem=i_ss.at[peer], recv_sem=i_rs.at[slot],
            device_id={"dp": peer}, device_id_type=MESH,
        )

    @pl.loop(1, n_dp)
    def _(s):
        i_copy((dp + s) % n_dp, dp).start()

    ibuf[dp] = folded

    for p in range(PARTS):
        y_copy(hi, p).wait_recv()
    own[hi] = own[hi] + ybuf[hi].astype(f32)

    @pl.loop(1, n_hi)
    def _(s):
        h = (hi + s) % n_hi
        for p in range(PARTS):
            z_copy(h, h, p).wait_recv()
        own[hi] = own[hi] + zbuf[h].astype(f32)

    first = dp * share
    src, start = first // depth, first % depth
    for g in range(groups):
        column = jnp.broadcast_to(mass[g : g + 1, :], (LANES, lane_len)).T + 1.0
        column = jnp.concatenate([column] * (width // LANES), axis=1)
        at = pl.ds(g * lane_len, lane_len)
        old = fc[src, pl.ds(pl.multiple_of(start + g * lane_len, lane_len), lane_len), :].astype(f32)
        new_ref[at, :] = ((own[hi, at, :] + old) / column).astype(bf16)

    @pl.loop(1, n_dp)
    def _(s):
        d = (dp + s) % n_dp
        i_copy(d, d).wait_recv()

    total = lax.fori_loop(1, n_dp, lambda d, t: t + ibuf[d], ibuf[0])
    inertia_ref[0, 0] = jnp.sum(total) / (rows * n_dp)

    for peer in peers:
        d_copy(peer, mp).wait_send()
        for c in range(CHUNKS):
            cent_copy(peer, mp, c).wait_send()

    @pl.loop(1, n_dp)
    def _(s):
        d = (dp + s) % n_dp
        i_copy(d, dp).wait_send()
        for copy in gather_copies(d, dp):
            copy.wait_send()

    @pl.loop(0, n_hi)
    def _(h):
        for p in range(PARTS):
            y_copy(h, p).wait_send()

    @pl.loop(1, n_hi)
    def _(s):
        for p in range(PARTS):
            z_copy((hi + s) % n_hi, hi, p).wait_send()


def per_device(n_dp, n_mp, documents, assign, quality, centroids):
    rows, width = documents.shape
    depth = centroids.shape[0]
    share = depth * n_mp // n_dp
    nb = rows // LANES
    n_hi = n_dp // 2
    lane_len = min(LANES, share)
    f32, bf16 = jnp.float32, jnp.bfloat16
    vmem = pl.BlockSpec(memory_space=pltpu.VMEM)
    dma = pltpu.SemaphoreType.DMA
    dist, new, cq, inertia = pl.pallas_call(
        functools.partial(kernel, n_dp, n_mp),
        out_shape=(
            jax.ShapeDtypeStruct((nb, LANES), f32),
            jax.ShapeDtypeStruct((share, width), bf16),
            jax.ShapeDtypeStruct((share // lane_len, lane_len), f32),
            jax.ShapeDtypeStruct((1, 1), f32),
        ),
        in_specs=[pl.BlockSpec(memory_space=pltpu.MemorySpace.HBM)] * 4,
        out_specs=(vmem, vmem, vmem, pl.BlockSpec(memory_space=pltpu.SMEM)),
        scratch_shapes=[
            pltpu.VMEM((nb, LANES), jnp.int32),
            pltpu.VMEM((nb, LANES), f32),
            pltpu.VMEM((rows, width), bf16),
            pltpu.VMEM((n_mp, depth, width), bf16),
            pltpu.VMEM((rows, width), f32),
            pltpu.VMEM((rows, LANES), f32),
            pltpu.VMEM((n_hi, share, width), f32),
            pltpu.VMEM((n_hi, share, width), bf16),
            pltpu.VMEM((n_hi, share, width), bf16),
            pltpu.VMEM((n_hi, share, width), bf16),
            pltpu.VMEM((n_hi, share, width), bf16),
            pltpu.VMEM((n_dp, nb, LANES), jnp.int32),
            pltpu.VMEM((n_dp, nb, LANES), f32),
            pltpu.VMEM((n_mp, nb, LANES), f32),
            pltpu.VMEM((n_dp, 8, LANES), f32),
            pltpu.VMEM((8, LANES), f32),
            dma((3,)), dma((n_mp, CHUNKS)), dma((n_mp, CHUNKS)), dma,
            dma((2, n_dp)), dma((2, n_dp)),
            dma((n_hi, PARTS)), dma((n_hi, PARTS)),
            dma((n_hi, PARTS)), dma((n_hi, PARTS)),
            dma((n_mp,)), dma((n_mp,)),
            dma((n_dp,)), dma((n_dp,)),
        ],
        compiler_params=pltpu.CompilerParams(
            collective_id=0, has_side_effects=True, vmem_limit_bytes=60 * 2**20
        ),
    )(assign.reshape(nb, LANES), quality.reshape(nb, LANES), documents, centroids)
    return dist.reshape(rows), new, cq.reshape(share), inertia.reshape(())


def solution(mesh):
    return jax.shard_map(
        functools.partial(per_device, mesh.shape["dp"], mesh.shape["mp"]),
        mesh=mesh,
        in_specs=(P("dp", "mp"), P("dp"), P("dp"), P("mp", None)),
        out_specs=(P("dp"), P("dp", "mp"), P("dp"), P()),
        check_vma=False,
    )
```
